32 devices in a mesh: dp: 4 (over x, core), rollout: 8 (over z, y).
Axes of the slice: x: 2, y: 2, z: 4, core: 2. Of those that a mesh axis runs over, the one named last changes fastest.
Arguments:
- queries: bfloat16 [32, 512, 2560], P(('dp', 'rollout')), may hold values from -100 to 100
- resp_keys: bfloat16 [32, 512, 512], P(('dp', 'rollout')), may hold values from -5 to 5
- resp_values: bfloat16 [32, 512, 512], P(('dp', 'rollout')), may hold values from -6 to 6
- prompt_keys: bfloat16 [4, 128, 512], P('dp', 'rollout'), may hold values from -6 to 6
- prompt_values: bfloat16 [4, 128, 512], P('dp', 'rollout'), may hold values from -6 to 6
- d_out: bfloat16 [32, 512, 2560], P(('dp', 'rollout')), may hold values from -6 to 6
- lengths: int32 [32], replicated, may hold values from 64 to 512
- owner: int32 [32], replicated, may hold values from 0 to 3
Outputs:
- attn_out: bfloat16 [32, 512, 2560], P(('dp', 'rollout'))
- d_queries: bfloat16 [32, 512, 2560], P(('dp', 'rollout'))
- d_resp_keys: bfloat16 [32, 512, 512], P(('dp', 'rollout'))
- d_resp_values: bfloat16 [32, 512, 512], P(('dp', 'rollout'))
- d_prompt_keys: float32 [4, 128, 512], P('dp', 'rollout')
- d_prompt_values: float32 [4, 128, 512], P('dp', 'rollout')
The draws below stay inside these ranges and needn't reach their ends.
Inputs may be any that keep to these rules, and one draw needn't show every extreme that they name: `lengths`: rows of a block at or past its length are padding.
All inputs are finite; a program needn't handle non-finite values.
Results may differ from the reference program's by a relative error of at most 0.0071.
Values may be sent and summed in bfloat16 or wider, within the bound.
A program may use at most 128 MiB of HBM per device.

```python
import jax
import jax.numpy as jnp
from jax import lax

HEAD_DIM = 128
BLOCK = 512
TILE = 128
QW = 2560
KW = 512
PROMPT = 128
NB = 32
N_DP = 4


def twin_keys(key):
    base = jax.random.normal(jax.random.fold_in(key, 11), (NB, BLOCK, KW), jnp.float32)
    base = jnp.clip(base, -4.0, 4.0)
    return base


def draw_resp_keys(key, part):
    return twin_keys(key).astype(jnp.bfloat16)


def draw_queries(key, part):
    base = jnp.clip(jax.random.normal(jax.random.fold_in(key, 23), (NB, BLOCK, QW), jnp.float32), -6.0, 6.0)
    return base.astype(jnp.bfloat16)


def touch_ends(entries, rng, least, top_value):
    place = [jax.random.randint(jax.random.fold_in(rng, axis), (), 0, length) for axis, length in enumerate(entries.shape)]
    longest = entries.shape.index(max(entries.shape))
    next_to = place[:longest] + [(place[longest] + 1) % entries.shape[longest]] + place[longest + 1:]
    return entries.at[tuple(place)].set(least).at[tuple(next_to)].set(top_value)


def levels(own_key, shape, shards, low, high):
    def one(position, parts):
        draws = jax.random.uniform(jax.random.fold_in(jax.random.fold_in(own_key, 6), position), (parts,), jnp.float32, low / len(shards), high / len(shards))
        return jnp.repeat(jnp.exp(draws), shape[position] // parts).reshape((-1,) + (1,) * (len(shape) - position - 1))

    level = one(*shards[0])
    for cut in shards[1:]:
        level = level * one(*cut)
    return level


def scatter_about(own_key, shape, width, most, split=(), kind=jnp.bfloat16):
    array = jax.random.normal(own_key, shape, jnp.float32) * width
    if len(split) > 0:
        array = levels(own_key, shape, split, -0.22, 0.18) * array
    return jnp.clip(array, min=-most, max=most).astype(kind)


def setup_inputs(seed: int = 0) -> dict:
    splits = jax.random.split(jax.random.key(seed), 9)
    queries = draw_queries(jax.random.fold_in(splits[8], 71), 0)
    resp_keys = draw_resp_keys(jax.random.fold_in(splits[8], 71), 0)
    resp_values = scatter_about(splits[2], (NB, BLOCK, KW), 1.0, 6.0, ((0, 32),))
    prompt_keys = scatter_about(splits[3], (N_DP, PROMPT, KW), 1.0, 6.0, ((0, 4), (1, 8)))
    prompt_values = scatter_about(splits[4], (N_DP, PROMPT, KW), 1.0, 6.0, ((0, 4), (1, 8)))
    d_out = scatter_about(splits[5], (NB, BLOCK, QW), 1.0, 6.0, ((0, 32),))
    lengths = touch_ends(jax.random.randint(splits[6], (NB,), BLOCK // 8, BLOCK + 1), jax.random.fold_in(splits[6], 1), BLOCK // 8, BLOCK).astype(jnp.int32)
    owner = touch_ends(jax.random.randint(splits[7], (NB,), 0, N_DP), jax.random.fold_in(splits[7], 1), 0, N_DP - 1).astype(jnp.int32)
    return dict(queries=queries, resp_keys=resp_keys, resp_values=resp_values, prompt_keys=prompt_keys, prompt_values=prompt_values, d_out=d_out, lengths=lengths, owner=owner)


def attend(q_rows, d_rows, offset, stride, length, keys, values):
    rows = q_rows.shape[0]
    span = keys.shape[0]
    kv_heads = keys.shape[1] // HEAD_DIM
    group = q_rows.shape[1] // keys.shape[1]
    key_heads = keys.astype(jnp.float32).reshape(span, kv_heads, HEAD_DIM)
    val_heads = values.astype(jnp.float32).reshape(span, kv_heads, HEAD_DIM)
    key_pos = jnp.arange(span, dtype=jnp.int32) - (span - BLOCK)
    live_rows = jnp.clip((length - offset + stride - 1) // stride, 0, rows)
    turns = ((live_rows + TILE - 1) // TILE).astype(jnp.int32)
    scale = HEAD_DIM ** -0.5

    def step(turn, carry):
        out_all, dq_all, dk_sum, dv_sum = carry
        start = (turn * TILE).astype(jnp.int32)
        qt = lax.dynamic_slice_in_dim(q_rows, start, TILE, 0).astype(jnp.float32)
        qt = qt.reshape(TILE, kv_heads, group, HEAD_DIM)
        dt = lax.dynamic_slice_in_dim(d_rows, start, TILE, 0)
        pos = offset + stride * (start + jnp.arange(TILE, dtype=jnp.int32))
        live = pos < length
        dt = jnp.where(live[:, None], dt, jnp.zeros_like(dt))
        dt = dt.astype(jnp.float32).reshape(TILE, kv_heads, group, HEAD_DIM)
        scores = jnp.einsum("tkgd,skd->kgts", qt, key_heads) * scale
        allowed = key_pos[None, :] <= pos[:, None]
        scores = jnp.where(allowed, scores, -1e30)
        top = jnp.max(scores, axis=-1, keepdims=True)
        expd = jnp.exp(scores - top)
        probs = expd / jnp.sum(expd, axis=-1, keepdims=True)
        weights = lax.optimization_barrier(probs.astype(jnp.bfloat16)).astype(jnp.float32)
        out = jnp.einsum("kgts,skd->tkgd", weights, val_heads)
        out = out * live.astype(jnp.float32)[:, None, None, None]
        dprob = jnp.einsum("tkgd,skd->kgts", dt, val_heads)
        delta = jnp.einsum("tkgd,tkgd->kgt", dt, out)
        dscore = probs * (dprob - delta[..., None]) * scale
        dscore = lax.optimization_barrier(dscore.astype(jnp.bfloat16)).astype(jnp.float32)
        dq = jnp.einsum("kgts,skd->tkgd", dscore, key_heads)
        dk_sum = dk_sum + jnp.einsum("kgts,tkgd->skd", dscore, qt)
        dv_sum = dv_sum + jnp.einsum("kgts,tkgd->skd", weights, dt)
        out_all = lax.dynamic_update_slice_in_dim(out_all, out.reshape(TILE, -1).astype(jnp.bfloat16), start, 0)
        dq_all = lax.dynamic_update_slice_in_dim(dq_all, dq.reshape(TILE, -1).astype(jnp.bfloat16), start, 0)
        return out_all, dq_all, dk_sum, dv_sum

    init = (jnp.zeros((rows, q_rows.shape[1]), jnp.bfloat16),
            jnp.zeros((rows, q_rows.shape[1]), jnp.bfloat16),
            jnp.zeros((span, kv_heads, HEAD_DIM), jnp.float32),
            jnp.zeros((span, kv_heads, HEAD_DIM), jnp.float32))
    out_all, dq_all, dk_sum, dv_sum = lax.fori_loop(jnp.int32(0), turns, step, init)
    return out_all, dq_all, dk_sum.reshape(span, -1), dv_sum.reshape(span, -1)


def reference(queries, resp_keys, resp_values, prompt_keys, prompt_values, d_out, lengths, owner):
    groups = prompt_keys.shape[0]
    prompt_n = prompt_keys.shape[1]
    width_k = prompt_keys.shape[2]

    def one(accum, index):
        own = owner[index]
        pkeys = lax.dynamic_index_in_dim(prompt_keys, own, 0, keepdims=False)
        pvals = lax.dynamic_index_in_dim(prompt_values, own, 0, keepdims=False)
        keys = jnp.concatenate([pkeys, resp_keys[index]], axis=0)
        values = jnp.concatenate([pvals, resp_values[index]], axis=0)
        out, dq, dk, dv = attend(queries[index], d_out[index], 0, 1, lengths[index], keys, values)
        select = (jnp.arange(groups, dtype=jnp.int32) == own).astype(jnp.float32)
        term = jnp.concatenate([dk[:prompt_n], dv[:prompt_n]], axis=1)
        accum = accum + select[:, None, None] * term[None]
        return accum, (out, dq, dk[prompt_n:].astype(jnp.bfloat16), dv[prompt_n:].astype(jnp.bfloat16))

    start = jnp.zeros((groups, prompt_n, 2 * width_k), jnp.float32)
    accum, results = lax.scan(one, start, jnp.arange(queries.shape[0], dtype=jnp.int32))
    return results[0], results[1], results[2], results[3], accum[..., :width_k], accum[..., width_k:]
```

```python
import functools
import math

import jax
import jax.numpy as jnp
from jax import lax
from jax.experimental import pallas as pl
from jax.experimental.pallas import tpu as pltpu
from jax.sharding import PartitionSpec as P

HEAD_DIM = 128
MESH = pl.DeviceIdType.MESH
ROWS = 256
VMEM = pltpu.VMEM


def greet(groups, shards):
    dp, ro = lax.axis_index("dp"), lax.axis_index("rollout")
    barrier = pltpu.get_barrier_semaphore()
    for k in range(1, groups):
        pl.semaphore_signal(
            barrier, inc=1, device_id={"dp": lax.rem(dp + k, groups)}, device_id_type=MESH
        )
    for k in range(1, shards):
        pl.semaphore_signal(
            barrier, inc=1, device_id={"rollout": lax.rem(ro + k, shards)}, device_id_type=MESH
        )
    pl.semaphore_wait(barrier, groups + shards - 2)


def gather_kernel(groups, shards, owner, pk, pv, out, mine, held, stage, s1, r1, s2, r2):
    dp, ro = lax.axis_index("dp"), lax.axis_index("rollout")
    n = mine.shape[1]
    mine[0] = pk[0]
    mine[1] = pv[0]
    greet(groups, shards)
    first = []
    for k in range(1, groups):
        copy = pltpu.make_async_remote_copy(
            src_ref=mine, dst_ref=held.at[k], send_sem=s1.at[k], recv_sem=r1.at[k],
            device_id={"dp": lax.rem(dp + k, groups)}, device_id_type=MESH,
        )
        copy.start()
        first.append(copy)
    held[0] = mine[...]
    for copy in first:
        copy.wait()

    def rows_of(peer):
        return held[lax.rem(dp - owner[dp * shards + peer] + groups, groups)]

    row = pl.ds(pl.multiple_of(ro * n, n), n)
    second = []
    for k in range(1, shards):
        peer = lax.rem(ro + k, shards)
        stage[k] = rows_of(peer)
        copy = pltpu.make_async_remote_copy(
            src_ref=stage.at[k], dst_ref=out.at[:, row, :], send_sem=s2.at[k], recv_sem=r2.at[k],
            device_id={"rollout": peer}, device_id_type=MESH,
        )
        copy.start()
        second.append(copy)
    out[:, row, :] = rows_of(ro)
    for copy in second:
        copy.wait()


def reduce_kernel(groups, shards, owner, term, dpk, dpv, got, acc, stage, got2, s1, r1, s2, r2):
    dp, ro = lax.axis_index("dp"), lax.axis_index("rollout")
    n = got.shape[2]
    greet(groups, shards)
    first = []
    for k in range(1, shards):
        peer = lax.rem(ro + k, shards)
        copy = pltpu.make_async_remote_copy(
            src_ref=term.at[:, pl.ds(pl.multiple_of(peer * n, n), n), :], dst_ref=got.at[k],
            send_sem=s1.at[k], recv_sem=r1.at[k],
            device_id={"rollout": peer}, device_id_type=MESH,
        )
        copy.start()
        first.append(copy)
    got[0] = term[:, pl.ds(pl.multiple_of(ro * n, n), n), :]
    for copy in first:
        copy.wait()
    for k in range(groups):
        target = lax.rem(dp + k, groups)
        total = jnp.zeros(acc.shape, jnp.float32)
        for j in range(shards):
            source = lax.rem(ro - j + shards, shards)
            pick = (owner[dp * shards + source] == target).astype(jnp.float32)
            total = total + pick * got[j].astype(jnp.float32)
        if k == 0:
            acc[...] = total
        else:
            stage[k] = total.astype(jnp.bfloat16)
    second = []
    for k in range(1, groups):
        copy = pltpu.make_async_remote_copy(
            src_ref=stage.at[k], dst_ref=got2.at[k], send_sem=s2.at[k], recv_sem=r2.at[k],
            device_id={"dp": lax.rem(dp + k, groups)}, device_id_type=MESH,
        )
        copy.start()
        second.append(copy)
    for copy in second:
        copy.wait()
    total = acc[...]
    for k in range(1, groups):
        total = total + got2[k].astype(jnp.float32)
    dpk[0] = total[0]
    dpv[0] = total[1]


def dot(a, b, dims=((1,), (0,))):
    return lax.dot_general(a, b, (dims, ((), ())), preferred_element_type=jnp.float32)


def attend_kernel(group, length, q, d, rk, rv, prompt, out, dq, dk, dv, term,
                  kc, vc, kt, vt, dks, dvs):
    block = q.shape[1]
    pn = prompt.shape[1]
    scale = HEAD_DIM ** -0.5
    live_n = length[0]
    kc[:pn] = prompt[0]
    kc[pn:] = rk[0]
    vc[:pn] = prompt[1]
    vc[pn:] = rv[0]
    kt[...] = kc[...].T
    vt[...] = vc[...].T
    dks[...] = jnp.zeros_like(dks)
    dvs[...] = jnp.zeros_like(dvs)
    lead = lax.broadcasted_iota(jnp.int32, (ROWS, ROWS), 0) <= lax.broadcasted_iota(
        jnp.int32, (ROWS, ROWS), 1
    )

    def head(h):
        cols = pl.ds(pl.multiple_of(h * HEAD_DIM, HEAD_DIM), HEAD_DIM)
        for t in range(block // ROWS):
            rows = pl.ds(t * ROWS, ROWS)
            old, span = pn + t * ROWS, pn + (t + 1) * ROWS
            live = (
                lax.broadcasted_iota(jnp.int32, (ROWS, HEAD_DIM), 0) + t * ROWS < live_n
            )
            qt = q[0, rows, cols]
            g = jnp.where(live, d[0, rows, cols].astype(jnp.float32), 0.0).astype(jnp.bfloat16)
            c = scale * math.log2(math.e)
            sa = dot(kc[:old], qt, ((1,), (1,))) * c
            sb = jnp.where(lead, dot(kc[old:span], qt, ((1,), (1,))) * c, -1e30)
            top = jnp.maximum(
                jnp.max(sa, axis=0, keepdims=True), jnp.max(sb, axis=0, keepdims=True)
            )
            ea, eb = jnp.exp2(sa - top), jnp.exp2(sb - top)
            inv = 1.0 / (
                jnp.sum(ea, axis=0, keepdims=True) + jnp.sum(eb, axis=0, keepdims=True)
            )
            p = jnp.concatenate([ea, eb], axis=0) * inv
            w = p.astype(jnp.bfloat16)
            o = dot(vt[:, :span], w)
            out[0, rows, cols] = jnp.where(live, o.T, 0.0).astype(jnp.bfloat16)
            dp = dot(vc[:span], g, ((1,), (1,)))
            delta = jnp.sum(p * dp, axis=0, keepdims=True)
            ds = (p * (dp - delta)).astype(jnp.bfloat16)
            dq[0, rows, cols] = (dot(kt[:, :span], ds) * scale).T.astype(jnp.bfloat16)
            dks[:span] += dot(ds, qt)
            dvs[:span] += dot(w, g)

    for h in range(group):
        head(h)
    dkf = dks[...] * scale
    dk[0] = dkf[pn:].astype(jnp.bfloat16)
    dv[0] = dvs[pn:].astype(jnp.bfloat16)
    term[0] = dkf[:pn].astype(jnp.bfloat16)
    term[1] = dvs[:pn].astype(jnp.bfloat16)


def per_device(queries, resp_keys, resp_values, prompt_keys, prompt_values, d_out, lengths, owner):
    shards = lax.axis_size("rollout")
    groups = lax.axis_size("dp")
    here = lax.axis_index("dp") * shards + lax.axis_index("rollout")
    n, kw = prompt_keys.shape[1:]
    pn = n * shards
    block, qw = queries.shape[1:]
    heads = kw // HEAD_DIM
    group = qw // kw
    span = pn + block
    smem = pl.BlockSpec(memory_space=pltpu.SMEM)
    vmem = pl.BlockSpec(memory_space=pltpu.VMEM)
    dma = pltpu.SemaphoreType.DMA
    bf16, f32 = jnp.bfloat16, jnp.float32

    prompt = pl.pallas_call(
        functools.partial(gather_kernel, groups, shards),
        out_shape=jax.ShapeDtypeStruct((2, pn, kw), bf16),
        in_specs=[smem, vmem, vmem],
        out_specs=vmem,
        scratch_shapes=[
            VMEM((2, n, kw), bf16), VMEM((groups, 2, n, kw), bf16), VMEM((shards, 2, n, kw), bf16),
            dma((groups,)), dma((groups,)), dma((shards,)), dma((shards,)),
        ],
        compiler_params=pltpu.CompilerParams(collective_id=0, has_side_effects=True),
        name="gather_prompt",
    )(owner, prompt_keys, prompt_values)

    wide = pl.BlockSpec((1, block, group * HEAD_DIM), lambda e: (0, 0, e))
    narrow = pl.BlockSpec((1, block, HEAD_DIM), lambda e: (0, 0, e))
    pair = pl.BlockSpec((2, pn, HEAD_DIM), lambda e: (0, 0, e))
    out, dq, dk, dv, term = pl.pallas_call(
        functools.partial(attend_kernel, group),
        grid=(heads,),
        out_shape=(
            jax.ShapeDtypeStruct(queries.shape, bf16),
            jax.ShapeDtypeStruct(queries.shape, bf16),
            jax.ShapeDtypeStruct(resp_keys.shape, bf16),
            jax.ShapeDtypeStruct(resp_keys.shape, bf16),
            jax.ShapeDtypeStruct((2, pn, kw), bf16),
        ),
        in_specs=[smem, wide, wide, narrow, narrow, pair],
        out_specs=(wide, wide, narrow, narrow, pair),
        scratch_shapes=[
            VMEM((span, HEAD_DIM), bf16), VMEM((span, HEAD_DIM), bf16),
            VMEM((HEAD_DIM, span), bf16), VMEM((HEAD_DIM, span), bf16),
            VMEM((span, HEAD_DIM), f32), VMEM((span, HEAD_DIM), f32),
        ],
        compiler_params=pltpu.CompilerParams(
            dimension_semantics=("arbitrary",), vmem_limit_bytes=56 * 1024 * 1024
        ),
        name="attend",
    )(lengths[here][None], queries, d_out, resp_keys, resp_values, prompt)

    shape = jax.ShapeDtypeStruct(prompt_keys.shape, f32)
    dpk, dpv = pl.pallas_call(
        functools.partial(reduce_kernel, groups, shards),
        out_shape=(shape, shape),
        in_specs=[smem, vmem],
        out_specs=(vmem, vmem),
        scratch_shapes=[
            VMEM((shards, 2, n, kw), bf16), VMEM((2, n, kw), f32),
            VMEM((groups, 2, n, kw), bf16), VMEM((groups, 2, n, kw), bf16),
            dma((shards,)), dma((shards,)), dma((groups,)), dma((groups,)),
        ],
        compiler_params=pltpu.CompilerParams(collective_id=1, has_side_effects=True),
        name="reduce_prompt",
    )(owner, term)
    return out, dq, dk, dv, dpk, dpv


def solution(mesh):
    rows = P(("dp", "rollout"), None, None)
    prompt = P("dp", "rollout", None)
    return jax.shard_map(
        per_device,
        mesh=mesh,
        in_specs=(rows, rows, rows, prompt, prompt, rows, P(), P()),
        out_specs=(rows, rows, rows, rows, prompt, prompt),
        check_vma=False,
    )
```
